128 devices in a mesh: rep: 8 (over y, z_hi), tp: 16 (over z_lo, x, core).
Axes of the slice: x: 4, y: 4, z: 4 (z_hi: 2, z_lo: 2; z = z_hi * 2 + z_lo), core: 2. Of those that a mesh axis runs over, the one named last changes fastest.
Arguments:
- residual: bfloat16 [8, 2048, 4096], P('rep', 'tp'), may hold values from -6 to 6
- gate_pre: bfloat16 [8, 2048, 7168], P('rep', None, 'tp'), may hold values from -6 to 6
- up_pre: bfloat16 [8, 2048, 7168], P('rep', None, 'tp'), may hold values from -6 to 6
- down_weight: bfloat16 [7168, 4096], P('tp'), may hold values from -0.0625 to 0.0625
- d_out: bfloat16 [8, 2048, 4096], P('rep', 'tp'), may hold values from -1.5 to 1.5
- comp_index: int32 [8, 112, 2048], P('rep', 'tp'), may hold values from 0 to 4095
- comp_value: bfloat16 [8, 112, 2048], P('rep', 'tp'), may hold values from -48 to 48
Outputs:
- output: bfloat16 [8, 2048, 4096], P('rep', 'tp')
- gate_preact_gradient: bfloat16 [8, 2048, 7168], P('rep', None, 'tp')
- up_grad: bfloat16 [8, 2048, 7168], P('rep', None, 'tp')
- weight_grad: bfloat16 [8, 7168, 4096], P('rep', 'tp')
- update: bfloat16 [7168, 4096], P('tp')
- updated_down_weight: bfloat16 [7168, 4096], P('tp')
The draws below stay inside these ranges and needn't reach their ends.
Inputs may be any that keep to these rules, and one draw needn't show every extreme that they name: `comp_index`: positions of one list may repeat.
All inputs are finite; a program needn't handle non-finite values.
Results may differ from the reference program's by a relative error of at most 0.011.
Values may be sent and summed in bfloat16 or wider, within the bound.
No kernel may reach another device: no remote copies, remote signals or barrier semaphores. Data moves between devices by JAX's collectives and lax.ppermute only.
A program may use at most 320 MiB of HBM per device.

```python
import jax
import jax.numpy as jnp
from jax import lax

D = 4096
FF = 7168
SPAN = 64
TOPK = 32
TOKENS = 2048
REPS = 8
N_REP = 8
N_TP = 16


def with_ends(drawn, key, least, largest):
    shape = drawn.shape
    spot = [jax.random.randint(jax.random.fold_in(key, axis), (), 0, shape[axis]) for axis in range(len(shape))]
    drawn = drawn.at[tuple(spot)].set(least)
    longest = shape.index(max(shape))
    spot[longest] = (spot[longest] + 1) % shape[longest]
    return drawn.at[tuple(spot)].set(largest)


def level_of(stream_key, shape, pieces, low, high):
    def one(dim, blocks):
        draws = jax.random.uniform(jax.random.fold_in(jax.random.fold_in(stream_key, 6), dim), (blocks,), jnp.float32, low / len(pieces), high / len(pieces))
        return jnp.repeat(jnp.exp(draws), shape[dim] // blocks).reshape((-1,) + (1,) * (len(shape) - dim - 1))

    level = one(*pieces[0])
    for cut in pieces[1:]:
        level = level * one(*cut)
    return level


def noise(key, extent, scale, bound, cuts=(), kind=jnp.bfloat16):
    drawn = scale * jax.random.normal(key, extent, jnp.float32)
    if cuts:
        drawn = drawn * level_of(key, extent, cuts, -0.22, 0.18)
    return jnp.clip(drawn, -bound, bound).astype(kind)


def setup_inputs(seed: int = 0) -> dict:
    keys = jax.random.split(jax.random.key(seed), 8)
    return {
        "residual": noise(keys[0], (REPS, TOKENS, D), 1.0, 6.0, ((0, 8), (1, 16))),
        "gate_pre": noise(keys[1], (REPS, TOKENS, FF), 1.0, 6.0, ((0, 8), (2, 16))),
        "up_pre": noise(keys[2], (REPS, TOKENS, FF), 1.0, 6.0, ((0, 8), (2, 16))),
        "down_weight": noise(keys[3], (FF, D), FF ** -0.5, 0.0625, ((0, 16),)),
        "d_out": noise(keys[4], (REPS, TOKENS, D), 0.25, 1.5, ((0, 8), (1, 16))),
        "comp_index": with_ends(jax.random.randint(keys[5], (REPS, FF // SPAN, (D // SPAN) * TOPK), 0, SPAN * SPAN), jax.random.fold_in(keys[5], 1), 0, (SPAN * SPAN) - 1).astype(jnp.int32),
        "comp_value": noise(keys[6], (REPS, FF // SPAN, (D // SPAN) * TOPK), 8.0, 48.0, ((0, 8), (1, 16))),
    }


def cosine_table(length):
    freq = jnp.arange(length, dtype=jnp.float32)[:, None]
    place = jnp.arange(length, dtype=jnp.float32)[None, :]
    scales = jnp.where(freq == 0, jnp.sqrt(1.0 / length), jnp.sqrt(2.0 / length))
    return scales * jnp.cos(jnp.pi * (2.0 * place + 1.0) * freq / (2.0 * length))

def reference(residual, gate_pre, up_pre, down_weight, d_out, comp_index, comp_value):
    units = FF // N_TP

    def per_replica(operands):
        residual_r, gate_r, up_r, grads_r = operands
        gate_f = gate_r.astype(jnp.float32)
        up_f = up_r.astype(jnp.float32)
        sigmoid_g = jax.nn.sigmoid(gate_f)
        activated = gate_f * sigmoid_g
        hidden = (activated * up_f).astype(jnp.bfloat16)
        summed = jnp.zeros((TOKENS, D), jnp.float32)
        for shard in range(N_TP):
            partial_out = jnp.dot(hidden[:, shard * units:(shard + 1) * units], down_weight[shard * units:(shard + 1) * units], preferred_element_type=jnp.float32)
            summed = summed + lax.optimization_barrier(partial_out.astype(jnp.bfloat16)).astype(jnp.float32)
        output = (residual_r.astype(jnp.float32) + summed).astype(jnp.bfloat16)
        hidden_grad = jnp.dot(grads_r, down_weight.T, preferred_element_type=jnp.float32)
        gate_preact_gradient = (hidden_grad * up_f * sigmoid_g * (1.0 + gate_f * (1.0 - sigmoid_g))).astype(jnp.bfloat16)
        up_grad = (hidden_grad * activated).astype(jnp.bfloat16)
        weight_grad = jnp.dot(hidden.T, grads_r, preferred_element_type=jnp.float32).astype(jnp.bfloat16)
        return (output, gate_preact_gradient, up_grad, weight_grad)
    output, gate_preact_gradient, up_grad, weight_grad = lax.map(per_replica, (residual, gate_pre, up_pre, d_out))
    cosine_basis = cosine_table(SPAN)
    columns = D // SPAN
    owners = jnp.broadcast_to((jnp.arange(columns * TOPK) // TOPK).astype(jnp.int32)[None, :], (N_REP, columns * TOPK))

    def span_row(operands):
        indices, amounts = operands
        flat = jnp.zeros((columns, SPAN * SPAN), jnp.float32).at[owners, indices.astype(jnp.int32)].add(amounts.astype(jnp.float32))
        spectral_coefficients = flat.reshape(columns, SPAN, SPAN)
        halfway_finished = jnp.einsum('kxt,ta->kxa', spectral_coefficients, cosine_basis, precision=lax.Precision.HIGHEST)
        output_block_list = jnp.einsum('nk,hnm->khm', cosine_basis, halfway_finished, precision=lax.Precision.HIGHEST)
        return output_block_list.reshape(SPAN, D)
    decoded = lax.map(span_row, (jnp.transpose(comp_index, (1, 0, 2)), jnp.transpose(comp_value, (1, 0, 2))))
    update = (decoded.reshape(FF, D) / N_REP).astype(jnp.bfloat16)
    updated_down_weight = (down_weight.astype(jnp.float32) - 0.02 * update.astype(jnp.float32)).astype(jnp.bfloat16)
    return (output, gate_preact_gradient, up_grad, weight_grad, update, updated_down_weight)
```

```python
import functools
import math

import jax
import jax.numpy as jnp
import numpy as np
from jax import lax
from jax.experimental import pallas as pl
from jax.experimental.pallas import tpu as pltpu
from jax.sharding import PartitionSpec as P


SPAN = 64
TOPK = 32
LEARN_RATE = 0.02
N_X = 4
N_Y = 4
TOK = 128


NT = (((1,), (1,)), ((), ()))


def tp_of(z, x, c):
    return (z * N_X + x % N_X) * 2 + c


TP = [(z, x, c) for z in range(2) for x in range(N_X) for c in range(2)]
TO_RIGHT = [(tp_of(z, x, c), tp_of(z, x + 1, c)) for z, x, c in TP]
TO_LEFT = [(tp_of(z, x, c), tp_of(z, x - 1, c)) for z, x, c in TP]
TO_Z = [(tp_of(z, x, c), tp_of(1 - z, x, c)) for z, x, c in TP]
TO_CORE = [(tp_of(z, x, c), tp_of(z, x, 1 - c)) for z, x, c in TP]
TO_UP = [(r, (r + 2) % 8) for r in range(8)]
TO_DOWN = [(r, (r - 2) % 8) for r in range(8)]
TO_FAR = [(r, (r + 4) % 8) for r in range(8)]
TO_HI = [(r, r ^ 1) for r in range(8)]
TO_BACK = [(r * 16 + t, (r ^ 1) * 16 + (t ^ 8)) for r in range(8) for t in range(16)]


def right(v):
    return lax.ppermute(v, "tp", TO_RIGHT)


def left(v):
    return lax.ppermute(v, "tp", TO_LEFT)


def over_z(v):
    return lax.ppermute(v, "tp", TO_Z)


def swap(v):
    return lax.ppermute(v, "tp", TO_CORE)


def cosine_table(length):
    freq = np.arange(length)[:, None]
    place = np.arange(length)[None, :]
    scales = np.where(freq == 0, math.sqrt(1.0 / length), math.sqrt(2.0 / length))
    return (scales * np.cos(np.pi * (2.0 * place + 1.0) * freq / (2.0 * length))).astype(np.float32)


def hidden_kernel(spots, g_any, u_any, other_any, own_any, g, u, h, sem_i, sem_o):
    n = g.shape[0]
    width = g.shape[2]
    half = n // 2
    loads = []
    for k in range(n):
        where = (1 - spots[9]) if k < half else spots[9]
        cols = pl.ds(pl.multiple_of(where * (half * width) + (k % half) * width, width), width)
        pair = [
            pltpu.make_async_copy(src.at[:, cols], dst.at[k], sem_i.at[i, k])
            for i, (src, dst) in enumerate(((g_any, g), (u_any, u)))
        ]
        for copy in pair:
            copy.start()
        loads.append(pair)
    stores = []
    for k in range(n):
        for copy in loads[k]:
            copy.wait()
        gf = g[k].astype(jnp.float32)
        h[k] = (gf * jax.nn.sigmoid(gf) * u[k].astype(jnp.float32)).astype(jnp.bfloat16)
        out = other_any if k < half else own_any
        store = pltpu.make_async_copy(h.at[k], out.at[:, (k % half) * width : (k % half + 1) * width], sem_o.at[k])
        store.start()
        stores.append(store)
    for store in stores:
        store.wait()


def hidden_halves(spots, gate_t, up_t):
    units, tokens = gate_t.shape
    n = 4
    any_spec = pl.BlockSpec(memory_space=pl.ANY)
    out = jax.ShapeDtypeStruct((units, tokens // 2), jnp.bfloat16)
    dma = pltpu.SemaphoreType.DMA
    return pl.pallas_call(
        hidden_kernel,
        grid_spec=pltpu.PrefetchScalarGridSpec(
            num_scalar_prefetch=1,
            grid=(),
            in_specs=[any_spec] * 2,
            out_specs=[any_spec] * 2,
            scratch_shapes=[pltpu.VMEM((n, units, tokens // n), jnp.bfloat16)] * 3 + [dma((2, n)), dma((n,))],
        ),
        out_shape=[out, out],
        compiler_params=pltpu.CompilerParams(vmem_limit_bytes=56 << 20),
        cost_estimate=pl.CostEstimate(flops=10 * units * tokens, bytes_accessed=6 * units * tokens, transcendentals=0),
        name="hidden_halves",
    )(spots, gate_t, up_t)


def grads_kernel(first, base, count, idx, *refs):
    refs = list(refs)
    pieces = [[refs.pop(0) for _ in range(n)] for n in count]
    w_any, g_any, u_any = refs.pop(0), refs.pop(0), refs.pop(0)
    if not first:
        acc_any = refs.pop(0)
        refs.pop(0)
        refs.pop(0)
    wg_any, pg_any, ug_any = refs.pop(0), refs.pop(0), refs.pop(0)
    d, w, g, u, acc, pgs, ugs, new = refs[:8]
    sem_d, sem_g, sem_o, sem_w, sem_c = refs[-5:]
    if not first:
        old = refs[8]
    pairs = len(count) // 2
    two = 2 * TOK
    core = idx[8]
    width = w.shape[1]
    chunk = 1024

    def lanes(k):
        return pl.ds(pl.multiple_of(idx[base + k] * two, two), two)

    def load_units(k):
        return (
            pltpu.make_async_copy(g_any.at[:, lanes(k)], g.at[k], sem_g.at[0, k]),
            pltpu.make_async_copy(u_any.at[:, lanes(k)], u.at[k], sem_g.at[1, k]),
        )

    def store_units(k):
        return (
            pltpu.make_async_copy(pgs.at[k], pg_any.at[:, lanes(k)], sem_o.at[0, k]),
            pltpu.make_async_copy(ugs.at[k], ug_any.at[:, lanes(k)], sem_o.at[1, k]),
        )

    weights = pltpu.make_async_copy(w_any, w, sem_w.at[0])
    if not first:
        before = pltpu.make_async_copy(acc_any, old, sem_w.at[1])

    def load_pair(k):
        for copy in load_units(k):
            copy.start()
        for side in range(2):
            at = 0
            where = core if side == 0 else 1 - core
            for piece in pieces[2 * k + side]:
                size = piece.shape[0]
                there = pl.ds(pl.multiple_of(k * two + where * TOK + at, 64), size)
                pltpu.make_async_copy(piece, d.at[there, :], sem_d.at[k, side]).start()
                at += size

    load_pair(0)
    weights.start()

    def wait_pair(k):
        for copy in load_units(k):
            copy.wait()
        for side in range(2):
            there = pl.ds(pl.multiple_of(k * two + side * TOK, TOK), TOK)
            pltpu.make_async_copy(w_any.at[0:TOK, :], d.at[there, :], sem_d.at[k, side]).wait()

    def units_of(k):
        gf = g[k].astype(jnp.float32)
        uf = u[k].astype(jnp.float32)
        s = jax.nn.sigmoid(gf)
        return gf, uf, s, gf * s

    def to_inputs(k, h, gf, uf, s, act):
        pgs[k] = (h * uf * s * (1.0 + gf * (1.0 - s))).astype(jnp.bfloat16)
        ugs[k] = (h * act).astype(jnp.bfloat16)
        for copy in store_units(k):
            copy.start()

    def one(k, _):
        wait_pair(k)
        for n in range(1, pairs):

            @pl.when(k == n - 1)
            def _(n=n):
                load_pair(n)
                if n == pairs - 1 and not first:
                    before.start()

        rows = pl.ds(pl.multiple_of(k * two, two), two)
        gf, uf, s, act = units_of(k)
        hid = (act * uf).astype(jnp.bfloat16)
        h = lax.dot_general(w[...], d[rows, :], NT, preferred_element_type=jnp.float32)
        for c in range(0, width, chunk):
            cols = slice(c, c + chunk)
            acc[:, cols] += jnp.dot(hid, d[rows, cols], preferred_element_type=jnp.float32)
        to_inputs(k, h, gf, uf, s, act)
        return 0

    acc[...] = jnp.zeros_like(acc)
    weights.wait()
    lax.fori_loop(0, pairs - 1, one, 0)
    k = pairs - 1
    wait_pair(k)
    if not first:
        before.wait()
    rows = slice(k * two, (k + 1) * two)
    gf, uf, s, act = units_of(k)
    hid = (act * uf).astype(jnp.bfloat16)
    stores = []
    for n, c in enumerate(range(0, width, chunk)):
        cols = slice(c, c + chunk)
        total = acc[:, cols] + jnp.dot(hid, d[rows, cols], preferred_element_type=jnp.float32)
        if not first:
            total = total + old[:, cols].astype(jnp.float32)
        new[:, cols] = total.astype(jnp.bfloat16)
        copy = pltpu.make_async_copy(new.at[:, cols], wg_any.at[:, cols], sem_c.at[n])
        copy.start()
        stores.append(copy)
    h = lax.dot_general(w[...], d[rows, :], NT, preferred_element_type=jnp.float32)
    to_inputs(k, h, gf, uf, s, act)
    for k in range(pairs):
        stores += store_units(k)
    for copy in stores:
        copy.wait()


def grads(base, idx, shards, w, gate_t, up_t, before=None):
    units, tokens = gate_t.shape
    width = w.shape[1]
    first = before is None
    count = [len(s) for s in shards]
    pairs = len(count) // 2
    two = 2 * TOK
    any_spec = pl.BlockSpec(memory_space=pl.ANY)
    args = [idx, *[v for s in shards for v in s], w, gate_t, up_t]
    aliases = {}
    bf, f32 = jnp.bfloat16, jnp.float32
    if not first:
        aliases = {len(args) + 1: 1, len(args) + 2: 2}
        args += list(before)
    scratch = [
        pltpu.VMEM((pairs * two, width), bf),
        pltpu.VMEM((units, width), bf),
        pltpu.VMEM((pairs, units, two), bf),
        pltpu.VMEM((pairs, units, two), bf),
        pltpu.VMEM((units, width), f32),
        pltpu.VMEM((pairs, units, two), bf),
        pltpu.VMEM((pairs, units, two), bf),
        pltpu.VMEM((units, width), bf),
    ]
    if not first:
        scratch += [pltpu.VMEM((units, width), bf)]
    dma = pltpu.SemaphoreType.DMA
    scratch += [dma((pairs, 2)), dma((2, pairs)), dma((2, pairs)), dma((2,)), dma((width // 1024,))]
    flat = jax.ShapeDtypeStruct((units, tokens), bf)
    return pl.pallas_call(
        functools.partial(grads_kernel, first, base, count),
        grid_spec=pltpu.PrefetchScalarGridSpec(
            num_scalar_prefetch=1,
            grid=(),
            in_specs=[any_spec] * (len(args) - 1),
            out_specs=[any_spec] * 3,
            scratch_shapes=scratch,
        ),
        out_shape=[jax.ShapeDtypeStruct((units, width), bf), flat, flat],
        input_output_aliases=aliases,
        compiler_params=pltpu.CompilerParams(vmem_limit_bytes=56 << 20),
        cost_estimate=pl.CostEstimate(flops=4 * units * width * pairs * two, bytes_accessed=24 << 20, transcendentals=0),
        name="grads_first" if first else "grads_second",
    )(*args)


def forward_kernel(count, pos, *refs):
    refs = list(refs)
    hiddens = [refs.pop(0) for _ in range(4)]
    w_refs = [refs.pop(0) for _ in range(count)]
    outs = [refs.pop(0) for _ in range(8)]
    lhs_t, lhs, w, out, sem_h, sem_w, sem_o = refs
    units = w_refs[0].shape[0]
    quarter = units // N_Y
    width = w_refs[0].shape[1] // 2
    bn = width // 2
    gets = []
    for r in range(4):
        cols = slice(r * TOK, (r + 1) * TOK)
        there = pl.ds(pl.multiple_of(pos[10 + r] * TOK, TOK), TOK)
        for n in range(2):
            to = lhs_t.at[n * units : (n + 1) * units, cols]
            gets.append(pltpu.make_async_copy(hiddens[n].at[:, there], to, sem_h.at[r, n]))
            for q in range(N_Y):
                base = (2 + n) * units + q * quarter
                rows = pl.ds(pl.multiple_of(pos[14 + q] * quarter, 16), quarter)
                to = lhs_t.at[base : base + quarter, cols]
                gets.append(pltpu.make_async_copy(hiddens[2 + n].at[rows, there], to, sem_h.at[r, 2 + N_Y * n + q]))
    for get in gets:
        get.start()
    loads = []
    for piece in range(4):
        at = 0
        cols = slice(piece * bn, (piece + 1) * bn)
        mine = []
        for n, r in enumerate(w_refs):
            mine.append(pltpu.make_async_copy(r.at[:, cols], w.at[piece, at : at + r.shape[0], :], sem_w.at[piece, n]))
            at += r.shape[0]
        loads.append(mine)
    for load in loads[0]:
        load.start()
    for get in gets:
        get.wait()
    lhs[...] = lhs_t[...].T
    puts = []
    step = 512
    for piece in range(4):
        half, off = piece // 2, piece % 2 * bn
        for load in loads[piece]:
            load.wait()
        if piece < 3:
            for load in loads[piece + 1]:
                load.start()

        def tile(j, _, piece=piece, half=half, off=off):
            here = pl.ds(pl.multiple_of(j * step, step), step)
            there = pl.ds(pl.multiple_of(off + j * step, step), step)
            out[half, :, there] = jnp.dot(lhs[...], w[piece, :, here], preferred_element_type=jnp.float32).astype(jnp.bfloat16)
            return 0

        lax.fori_loop(0, bn // step, tile, 0)
        for r in range(4):
            cols = slice(off, off + bn)
            put = pltpu.make_async_copy(
                out.at[half, r * TOK : (r + 1) * TOK, cols], outs[4 * half + r].at[:, cols], sem_o.at[piece, r]
            )
            put.start()
            puts.append(put)
    for put in puts:
        put.wait()


def forward(pos, hiddens, weights):
    units, _ = hiddens[0].shape
    width = weights[0].shape[1] // 2
    any_spec = pl.BlockSpec(memory_space=pl.ANY)
    part = jax.ShapeDtypeStruct((TOK, width), jnp.bfloat16)
    bf = jnp.bfloat16
    dma = pltpu.SemaphoreType.DMA
    parts = pl.pallas_call(
        functools.partial(forward_kernel, len(weights)),
        grid_spec=pltpu.PrefetchScalarGridSpec(
            num_scalar_prefetch=1,
            grid=(),
            in_specs=[any_spec] * (4 + len(weights)),
            out_specs=[any_spec] * 8,
            scratch_shapes=[
                pltpu.VMEM((4 * units, 4 * TOK), bf),
                pltpu.VMEM((4 * TOK, 4 * units), bf),
                pltpu.VMEM((4, 4 * units, width // 2), bf),
                pltpu.VMEM((2, 4 * TOK, width), bf),
                dma((4, 2 + 2 * N_Y)),
                dma((4, len(weights))),
                dma((4, 4)),
            ],
        ),
        out_shape=[part] * 8,
        compiler_params=pltpu.CompilerParams(vmem_limit_bytes=56 << 20),
        cost_estimate=pl.CostEstimate(flops=2 * 4 * TOK * 4 * units * 2 * width, bytes_accessed=22 << 20, transcendentals=0),
        name="forward",
    )(pos, *hiddens, *weights)
    return parts[:4], parts[4:]


def decode_kernel(comp_a, comp_b, comp_c, comp_d, wv, cos_ref, ct_ref, upv, newv, cb_ref, fields, co4, mid):
    bf, f32 = jnp.bfloat16, jnp.float32
    a = pl.program_id(0)
    comps = [ref.at[n] for ref in (comp_a, comp_b, comp_c, comp_d) for n in range(ref.shape[0])]
    replicas = len(comps)
    per = 128 // TOPK
    groups = fields.shape[2]
    rows = fields.shape[1] // 3
    count = replicas * TOPK

    @pl.when(a == 0)
    def _():
        cb_ref[...] = jnp.zeros_like(cb_ref)
        for bl in range(per):
            here = slice(bl * SPAN, (bl + 1) * SPAN)
            cb_ref[here, here] = cos_ref[...]
        lane = lax.broadcasted_iota(jnp.int32, (128, count), 0)
        out = lax.broadcasted_iota(jnp.int32, (128, count), 1)
        for bl in range(per):
            total = None
            for r in range(replicas):
                pick = ((lane == bl * TOPK + out - r * TOPK) & (out // TOPK == r)).astype(f32).astype(bf)
                part = jnp.dot(comps[r][...], pick, preferred_element_type=f32)
                total = part if total is None else total + part
            fields[bl] = total.reshape(fields.shape[1:])

    spot = lax.broadcasted_iota(jnp.int32, (SPAN, count), 0).astype(f32)

    def group(g, _):
        four = []
        for bl in range(per):
            at = pl.ds(g, 1)
            i = fields[bl, a, at, :]
            j = fields[bl, rows + a, at, :]
            v = fields[bl, 2 * rows + a, at, :]
            left_hot = jnp.where(spot == i, v, 0.0).astype(bf)
            right_hot = jnp.where(spot == j, 1.0, 0.0).astype(bf)
            four.append(lax.dot_general(left_hot, right_hot, NT, preferred_element_type=f32))
        co4[pl.ds(pl.multiple_of(g * SPAN, SPAN), SPAN), :] = jnp.concatenate(four, axis=1).astype(bf)
        return 0

    lax.fori_loop(0, groups, group, 0, unroll=16)
    mid[...] = jnp.dot(co4[...], cb_ref[...], preferred_element_type=f32).astype(bf)
    step = per * SPAN
    for g in range(groups):
        cols = slice(g * step, (g + 1) * step)
        block = jnp.dot(ct_ref[...], mid[g * SPAN : (g + 1) * SPAN, :], preferred_element_type=f32)
        update = block.astype(bf)
        upv[:, cols] = update
        newv[:, cols] = (wv[:, cols].astype(f32) - LEARN_RATE * update.astype(f32)).astype(bf)


def decode(comp, w):
    replicas = sum(v.shape[0] for v in comp)
    width = w.shape[1]
    rows = w.shape[0] // SPAN
    per = 128 // TOPK
    groups = width // SPAN // per
    cos = cosine_table(SPAN)
    cb = jnp.asarray(cos, jnp.bfloat16)
    ct = jnp.asarray(cos.T / replicas, jnp.bfloat16)
    whole = lambda v: pl.BlockSpec(v.shape, lambda a: (0,) * v.ndim)
    wide = pl.BlockSpec((SPAN, width), lambda a: (a, 0))
    out = jax.ShapeDtypeStruct(w.shape, jnp.bfloat16)
    bf = jnp.bfloat16
    return pl.pallas_call(
        decode_kernel,
        grid=(rows,),
        in_specs=[*[whole(v) for v in comp], wide, whole(cb), whole(ct)],
        out_specs=[wide, wide],
        out_shape=[out, out],
        scratch_shapes=[
            pltpu.VMEM((per * SPAN, per * SPAN), bf),
            pltpu.VMEM((per, 3 * rows, groups, replicas * TOPK), jnp.float32),
            pltpu.VMEM((groups * SPAN, per * SPAN), bf),
            pltpu.VMEM((groups * SPAN, per * SPAN), bf),
        ],
        cost_estimate=pl.CostEstimate(flops=8 << 30, bytes_accessed=12 << 20, transcendentals=0),
        name="decode",
    )(*comp, w, cb, ct)


def everyones_components(comp_index, comp_value):
    index = comp_index[0]
    mine = jnp.concatenate(
        [(index // SPAN).astype(jnp.bfloat16), (index % SPAN).astype(jnp.bfloat16), comp_value[0]], axis=0
    )
    mine = mine.reshape(-1, 128)
    pair = jnp.stack([mine, lax.ppermute(mine, "rep", TO_HI)])
    return [pair] + [lax.ppermute(pair, "rep", to) for to in (TO_UP, TO_DOWN, TO_FAR)]


def body(residual, gate_pre, up_pre, down_weight, d_out, comp_index, comp_value):
    t = lax.axis_index("tp")
    z, x, c = t // (2 * N_X), (t // 2) % N_X, t % 2
    y = lax.axis_index("rep") // 2
    gate_t = jnp.swapaxes(gate_pre[0], 0, 1)
    up_t = jnp.swapaxes(up_pre[0], 0, 1)
    w = down_weight
    quarter = w.shape[0] // N_Y
    own = d_out[0]

    steps = ((0, 0), (1, 0), (0, 3), (0, 1), (0, 2), (1, 3), (1, 1), (1, 2))
    spots = jnp.stack(
        [(z if dz == 0 else 1 - z) * N_X + (x + dx) % N_X for dz, dx in steps]
        + [c, z]
        + [((x + r) % N_X) * 2 + c for r in (2, 1, 3, 0)]
        + [(y + q) % N_Y for q in (0, 3, 1, 2)]
    ).astype(jnp.int32)

    from_z = over_z(own)
    from_l = right(own)
    from_r = left(own)
    own_p = swap(own)
    w_q0 = lax.ppermute(lax.dynamic_slice_in_dim(w, y * quarter, quarter, 0), ("rep", "tp"), TO_BACK)
    far_q = (y + N_Y // 2) % N_Y
    w_q2 = lax.ppermute(lax.dynamic_slice_in_dim(w, far_q * quarter, quarter, 0), ("rep", "tp"), TO_BACK)
    w_p = swap(w)
    comp = everyones_components(comp_index, comp_value)
    hid_other, hid_own = hidden_halves(spots, gate_t, up_t)
    hz = over_z(hid_other)
    hs_p = swap(hid_own)
    hz_p = swap(hz)

    update, updated = decode(comp, w)

    half_rows = TOK // 2
    cut_a = from_l[:half_rows]
    cut_b = from_r[half_rows:]
    far_a = right(cut_a)
    far_b = left(cut_b)
    from_zl = right(from_z)
    from_zr = left(from_z)
    from_zfar_a = over_z(far_a)
    from_zfar_b = over_z(far_b)

    near = [[own], [own_p], [from_z], [swap(from_z)]]
    near += [[from_l], [swap(from_l)], [from_r], [swap(from_r)]]
    before = grads(0, spots, near, w, gate_t, up_t)
    rest = [[far_a, far_b], [swap(far_a), swap(far_b)]]
    rest += [[from_zl], [swap(from_zl)], [from_zr], [swap(from_zr)]]
    rest += [[from_zfar_a, from_zfar_b], [swap(from_zfar_a), swap(from_zfar_b)]]
    weight_grad, pre_grad, up_grad = grads(
        4, spots, rest, w, gate_t, up_t, before
    )

    width = w.shape[1] // 2
    w_qm = lax.ppermute(w_q0, "rep", TO_UP)
    w_qp = lax.ppermute(w_q0, "rep", TO_DOWN)
    w_back = [w_q0, w_qm, w_qp, w_q2]
    weights = [w, w_p, *w_back, *[swap(v) for v in w_back]]
    (a2, a1, a3, a0), (b2, b1, b3, b0) = forward(spots, (hid_own, hs_p, hz, hz_p), weights)
    f32 = jnp.float32

    ra = right(a2)
    rb = left(b2)
    ga = left(a3)
    gb = right(b1)
    sum_a = (a1.astype(f32) + ra.astype(f32)).astype(jnp.bfloat16)
    sum_b = (b3.astype(f32) + rb.astype(f32)).astype(jnp.bfloat16)
    fa = right(sum_a)
    fb = left(sum_b)
    res = residual[0]
    out_a = res[:, :width].astype(f32) + a0.astype(f32) + ga.astype(f32) + fa.astype(f32)
    out_b = res[:, width:].astype(f32) + b0.astype(f32) + gb.astype(f32) + fb.astype(f32)
    output = jnp.concatenate([out_a, out_b], axis=1).astype(jnp.bfloat16)
    return (
        output[None],
        jnp.swapaxes(pre_grad, 0, 1)[None],
        jnp.swapaxes(up_grad, 0, 1)[None],
        weight_grad[None],
        update,
        updated,
    )


def solution(mesh):
    return jax.shard_map(
        body,
        mesh=mesh,
        in_specs=(
            P("rep", "tp", None),
            P("rep", None, "tp"),
            P("rep", None, "tp"),
            P("tp", None),
            P("rep", "tp", None),
            P("rep", "tp", None),
            P("rep", "tp", None),
        ),
        out_specs=(
            P("rep", "tp", None),
            P("rep", None, "tp"),
            P("rep", None, "tp"),
            P("rep", "tp", None),
            P("tp", None),
            P("tp", None),
        ),
        check_vma=False,
    )
```

```python
import functools
import math

import jax
import jax.numpy as jnp
import numpy as np
from jax import lax
from jax.experimental import pallas as pl
from jax.experimental.pallas import tpu as pltpu
from jax.sharding import PartitionSpec as P


SPAN = 64
TOPK = 32
LEARN_RATE = 0.02
N_X = 4
N_Y = 4
TOK = 128


NT = (((1,), (1,)), ((), ()))


def tp_of(z, x, c):
    return (z * N_X + x % N_X) * 2 + c


TP = [(z, x, c) for z in range(2) for x in range(N_X) for c in range(2)]
TO_RIGHT = [(tp_of(z, x, c), tp_of(z, x + 1, c)) for z, x, c in TP]
TO_LEFT = [(tp_of(z, x, c), tp_of(z, x - 1, c)) for z, x, c in TP]
TO_Z = [(tp_of(z, x, c), tp_of(1 - z, x, c)) for z, x, c in TP]
TO_CORE = [(tp_of(z, x, c), tp_of(z, x, 1 - c)) for z, x, c in TP]
TO_UP = [(r, (r + 2) % 8) for r in range(8)]
TO_DOWN = [(r, (r - 2) % 8) for r in range(8)]
TO_FAR = [(r, (r + 4) % 8) for r in range(8)]
TO_HI = [(r, r ^ 1) for r in range(8)]
TO_BACK = [(r * 16 + t, (r ^ 1) * 16 + (t ^ 8)) for r in range(8) for t in range(16)]


def right(v):
    return lax.ppermute(v, "tp", TO_RIGHT)


def left(v):
    return lax.ppermute(v, "tp", TO_LEFT)


def over_z(v):
    return lax.ppermute(v, "tp", TO_Z)


def swap(v):
    return lax.ppermute(v, "tp", TO_CORE)


def cosine_table(length):
    freq = np.arange(length)[:, None]
    place = np.arange(length)[None, :]
    scales = np.where(freq == 0, math.sqrt(1.0 / length), math.sqrt(2.0 / length))
    return (scales * np.cos(np.pi * (2.0 * place + 1.0) * freq / (2.0 * length))).astype(np.float32)


def hidden_kernel(spots, g_any, u_any, other_any, own_any, g, u, h, sem_i, sem_o):
    n = g.shape[0]
    width = g.shape[2]
    half = n // 2
    loads = []
    for k in range(n):
        where = (1 - spots[9]) if k < half else spots[9]
        cols = pl.ds(pl.multiple_of(where * (half * width) + (k % half) * width, width), width)
        pair = [
            pltpu.make_async_copy(src.at[:, cols], dst.at[k], sem_i.at[i, k])
            for i, (src, dst) in enumerate(((g_any, g), (u_any, u)))
        ]
        for copy in pair:
            copy.start()
        loads.append(pair)
    stores = []
    for k in range(n):
        for copy in loads[k]:
            copy.wait()
        gf = g[k].astype(jnp.float32)
        h[k] = (gf * jax.nn.sigmoid(gf) * u[k].astype(jnp.float32)).astype(jnp.bfloat16)
        out = other_any if k < half else own_any
        store = pltpu.make_async_copy(h.at[k], out.at[:, (k % half) * width : (k % half + 1) * width], sem_o.at[k])
        store.start()
        stores.append(store)
    for store in stores:
        store.wait()


def hidden_halves(spots, gate_t, up_t):
    units, tokens = gate_t.shape
    n = 4
    any_spec = pl.BlockSpec(memory_space=pl.ANY)
    out = jax.ShapeDtypeStruct((units, tokens // 2), jnp.bfloat16)
    dma = pltpu.SemaphoreType.DMA
    return pl.pallas_call(
        hidden_kernel,
        grid_spec=pltpu.PrefetchScalarGridSpec(
            num_scalar_prefetch=1,
            grid=(),
            in_specs=[any_spec] * 2,
            out_specs=[any_spec] * 2,
            scratch_shapes=[pltpu.VMEM((n, units, tokens // n), jnp.bfloat16)] * 3 + [dma((2, n)), dma((n,))],
        ),
        out_shape=[out, out],
        compiler_params=pltpu.CompilerParams(vmem_limit_bytes=56 << 20),
        cost_estimate=pl.CostEstimate(flops=10 * units * tokens, bytes_accessed=6 * units * tokens, transcendentals=0),
        name="hidden_halves",
    )(spots, gate_t, up_t)


def grads_kernel(first, base, count, idx, *refs):
    refs = list(refs)
    pieces = [[refs.pop(0) for _ in range(n)] for n in count]
    w_any, g_any, u_any = refs.pop(0), refs.pop(0), refs.pop(0)
    if not first:
        acc_any = refs.pop(0)
        refs.pop(0)
        refs.pop(0)
    wg_any, pg_any, ug_any = refs.pop(0), refs.pop(0), refs.pop(0)
    d, w, g, u, acc, pgs, ugs, new = refs[:8]
    sem_d, sem_g, sem_o, sem_w, sem_c = refs[-5:]
    if not first:
        old = refs[8]
    pairs = len(count) // 2
    two = 2 * TOK
    core = idx[8]
    width = w.shape[1]
    chunk = 1024

    def lanes(k):
        return pl.ds(pl.multiple_of(idx[base + k] * two, two), two)

    def load_units(k):
        return (
            pltpu.make_async_copy(g_any.at[:, lanes(k)], g.at[k], sem_g.at[0, k]),
            pltpu.make_async_copy(u_any.at[:, lanes(k)], u.at[k], sem_g.at[1, k]),
        )

    def store_units(k):
        return (
            pltpu.make_async_copy(pgs.at[k], pg_any.at[:, lanes(k)], sem_o.at[0, k]),
            pltpu.make_async_copy(ugs.at[k], ug_any.at[:, lanes(k)], sem_o.at[1, k]),
        )

    weights = pltpu.make_async_copy(w_any, w, sem_w.at[0])
    if not first:
        before = pltpu.make_async_copy(acc_any, old, sem_w.at[1])

    def load_pair(k):
        for copy in load_units(k):
            copy.start()
        for side in range(2):
            at = 0
            where = core if side == 0 else 1 - core
            for piece in pieces[2 * k + side]:
                size = piece.shape[0]
                there = pl.ds(pl.multiple_of(k * two + where * TOK + at, 64), size)
                pltpu.make_async_copy(piece, d.at[there, :], sem_d.at[k, side]).start()
                at += size

    load_pair(0)
    weights.start()

    def wait_pair(k):
        for copy in load_units(k):
            copy.wait()
        for side in range(2):
            there = pl.ds(pl.multiple_of(k * two + side * TOK, TOK), TOK)
            pltpu.make_async_copy(w_any.at[0:TOK, :], d.at[there, :], sem_d.at[k, side]).wait()

    def units_of(k):
        gf = g[k].astype(jnp.float32)
        uf = u[k].astype(jnp.float32)
        s = jax.nn.sigmoid(gf)
        return gf, uf, s, gf * s

    def to_inputs(k, h, gf, uf, s, act):
        pgs[k] = (h * uf * s * (1.0 + gf * (1.0 - s))).astype(jnp.bfloat16)
        ugs[k] = (h * act).astype(jnp.bfloat16)
        for copy in store_units(k):
            copy.start()

    def one(k, _):
        wait_pair(k)
        for n in range(1, pairs):

            @pl.when(k == n - 1)
            def _(n=n):
                load_pair(n)
                if n == pairs - 1 and not first:
                    before.start()

        rows = pl.ds(pl.multiple_of(k * two, two), two)
        gf, uf, s, act = units_of(k)
        hid = (act * uf).astype(jnp.bfloat16)
        h = lax.dot_general(w[...], d[rows, :], NT, preferred_element_type=jnp.float32)
        for c in range(0, width, chunk):
            cols = slice(c, c + chunk)
            acc[:, cols] += jnp.dot(hid, d[rows, cols], preferred_element_type=jnp.float32)
        to_inputs(k, h, gf, uf, s, act)
        return 0

    acc[...] = jnp.zeros_like(acc)
    weights.wait()
    lax.fori_loop(0, pairs - 1, one, 0)
    k = pairs - 1
    wait_pair(k)
    if not first:
        before.wait()
    rows = slice(k * two, (k + 1) * two)
    gf, uf, s, act = units_of(k)
    hid = (act * uf).astype(jnp.bfloat16)
    stores = []
    for n, c in enumerate(range(0, width, chunk)):
        cols = slice(c, c + chunk)
        total = acc[:, cols] + jnp.dot(hid, d[rows, cols], preferred_element_type=jnp.float32)
        if not first:
            total = total + old[:, cols].astype(jnp.float32)
        new[:, cols] = total.astype(jnp.bfloat16)
        copy = pltpu.make_async_copy(new.at[:, cols], wg_any.at[:, cols], sem_c.at[n])
        copy.start()
        stores.append(copy)
    h = lax.dot_general(w[...], d[rows, :], NT, preferred_element_type=jnp.float32)
    to_inputs(k, h, gf, uf, s, act)
    for k in range(pairs):
        stores += store_units(k)
    for copy in stores:
        copy.wait()


def grads(base, idx, shards, w, gate_t, up_t, before=None):
    units, tokens = gate_t.shape
    width = w.shape[1]
    first = before is None
    count = [len(s) for s in shards]
    pairs = len(count) // 2
    two = 2 * TOK
    any_spec = pl.BlockSpec(memory_space=pl.ANY)
    args = [idx, *[v for s in shards for v in s], w, gate_t, up_t]
    aliases = {}
    bf, f32 = jnp.bfloat16, jnp.float32
    if not first:
        aliases = {len(args) + 1: 1, len(args) + 2: 2}
        args += list(before)
    scratch = [
        pltpu.VMEM((pairs * two, width), bf),
        pltpu.VMEM((units, width), bf),
        pltpu.VMEM((pairs, units, two), bf),
        pltpu.VMEM((pairs, units, two), bf),
        pltpu.VMEM((units, width), f32),
        pltpu.VMEM((pairs, units, two), bf),
        pltpu.VMEM((pairs, units, two), bf),
        pltpu.VMEM((units, width), bf),
    ]
    if not first:
        scratch += [pltpu.VMEM((units, width), bf)]
    dma = pltpu.SemaphoreType.DMA
    scratch += [dma((pairs, 2)), dma((2, pairs)), dma((2, pairs)), dma((2,)), dma((width // 1024,))]
    flat = jax.ShapeDtypeStruct((units, tokens), bf)
    return pl.pallas_call(
        functools.partial(grads_kernel, first, base, count),
        grid_spec=pltpu.PrefetchScalarGridSpec(
            num_scalar_prefetch=1,
            grid=(),
            in_specs=[any_spec] * (len(args) - 1),
            out_specs=[any_spec] * 3,
            scratch_shapes=scratch,
        ),
        out_shape=[jax.ShapeDtypeStruct((units, width), bf), flat, flat],
        input_output_aliases=aliases,
        compiler_params=pltpu.CompilerParams(vmem_limit_bytes=56 << 20),
        cost_estimate=pl.CostEstimate(flops=4 * units * width * pairs * two, bytes_accessed=24 << 20, transcendentals=0),
        name="grads_first" if first else "grads_second",
    )(*args)


def forward_kernel(count, pos, *refs):
    refs = list(refs)
    hiddens = [refs.pop(0) for _ in range(4)]
    w_refs = [refs.pop(0) for _ in range(count)]
    outs = [refs.pop(0) for _ in range(8)]
    lhs_t, lhs, w, out, sem_h, sem_w, sem_o = refs
    units = w_refs[0].shape[0]
    quarter = units // N_Y
    width = w_refs[0].shape[1] // 2
    bn = width // 2
    gets = []
    for r in range(4):
        cols = slice(r * TOK, (r + 1) * TOK)
        there = pl.ds(pl.multiple_of(pos[10 + r] * TOK, TOK), TOK)
        for n in range(2):
            to = lhs_t.at[n * units : (n + 1) * units, cols]
            gets.append(pltpu.make_async_copy(hiddens[n].at[:, there], to, sem_h.at[r, n]))
            for q in range(N_Y):
                base = (2 + n) * units + q * quarter
                rows = pl.ds(pl.multiple_of(pos[14 + q] * quarter, 16), quarter)
                to = lhs_t.at[base : base + quarter, cols]
                gets.append(pltpu.make_async_copy(hiddens[2 + n].at[rows, there], to, sem_h.at[r, 2 + N_Y * n + q]))
    for get in gets:
        get.start()
    loads = []
    for piece in range(4):
        at = 0
        cols = slice(piece * bn, (piece + 1) * bn)
        mine = []
        for n, r in enumerate(w_refs):
            mine.append(pltpu.make_async_copy(r.at[:, cols], w.at[piece, at : at + r.shape[0], :], sem_w.at[piece, n]))
            at += r.shape[0]
        loads.append(mine)
    for load in loads[0]:
        load.start()
    for get in gets:
        get.wait()
    lhs[...] = lhs_t[...].T
    puts = []
    step = 512
    for piece in range(4):
        half, off = piece // 2, piece % 2 * bn
        for load in loads[piece]:
            load.wait()
        if piece < 3:
            for load in loads[piece + 1]:
                load.start()

        def tile(j, _, piece=piece, half=half, off=off):
            here = pl.ds(pl.multiple_of(j * step, step), step)
            there = pl.ds(pl.multiple_of(off + j * step, step), step)
            out[half, :, there] = jnp.dot(lhs[...], w[piece, :, here], preferred_element_type=jnp.float32).astype(jnp.bfloat16)
            return 0

        lax.fori_loop(0, bn // step, tile, 0)
        for r in range(4):
            cols = slice(off, off + bn)
            put = pltpu.make_async_copy(
                out.at[half, r * TOK : (r + 1) * TOK, cols], outs[4 * half + r].at[:, cols], sem_o.at[piece, r]
            )
            put.start()
            puts.append(put)
    for put in puts:
        put.wait()


def forward(pos, hiddens, weights):
    units, _ = hiddens[0].shape
    width = weights[0].shape[1] // 2
    any_spec = pl.BlockSpec(memory_space=pl.ANY)
    part = jax.ShapeDtypeStruct((TOK, width), jnp.bfloat16)
    bf = jnp.bfloat16
    dma = pltpu.SemaphoreType.DMA
    parts = pl.pallas_call(
        functools.partial(forward_kernel, len(weights)),
        grid_spec=pltpu.PrefetchScalarGridSpec(
            num_scalar_prefetch=1,
            grid=(),
            in_specs=[any_spec] * (4 + len(weights)),
            out_specs=[any_spec] * 8,
            scratch_shapes=[
                pltpu.VMEM((4 * units, 4 * TOK), bf),
                pltpu.VMEM((4 * TOK, 4 * units), bf),
                pltpu.VMEM((4, 4 * units, width // 2), bf),
                pltpu.VMEM((2, 4 * TOK, width), bf),
                dma((4, 2 + 2 * N_Y)),
                dma((4, len(weights))),
                dma((4, 4)),
            ],
        ),
        out_shape=[part] * 8,
        compiler_params=pltpu.CompilerParams(vmem_limit_bytes=56 << 20),
        cost_estimate=pl.CostEstimate(flops=2 * 4 * TOK * 4 * units * 2 * width, bytes_accessed=22 << 20, transcendentals=0),
        name="forward",
    )(pos, *hiddens, *weights)
    return parts[:4], parts[4:]


def decode_kernel(base, comp_a, comp_b, comp_c, comp_d, wv, cos_ref, ct_ref, *refs):
    upv, newv, cb_ref, fields, co4, mid = refs[-6:]
    bf, f32 = jnp.bfloat16, jnp.float32
    a = pl.program_id(0) + base
    comps = [ref.at[n] for ref in (comp_a, comp_b, comp_c, comp_d) for n in range(ref.shape[0])]
    replicas = len(comps)
    per = 128 // TOPK
    groups = fields.shape[2]
    rows = fields.shape[1] // 3
    count = replicas * TOPK

    @pl.when(a == base)
    def _():
        cb_ref[...] = jnp.zeros_like(cb_ref)
        for bl in range(per):
            here = slice(bl * SPAN, (bl + 1) * SPAN)
            cb_ref[here, here] = cos_ref[...]
        lane = lax.broadcasted_iota(jnp.int32, (128, count), 0)
        out = lax.broadcasted_iota(jnp.int32, (128, count), 1)
        for bl in range(per):
            total = None
            for r in range(replicas):
                pick = ((lane == bl * TOPK + out - r * TOPK) & (out // TOPK == r)).astype(f32).astype(bf)
                part = jnp.dot(comps[r][...], pick, preferred_element_type=f32)
                total = part if total is None else total + part
            fields[bl] = total.reshape(fields.shape[1:])

    spot = lax.broadcasted_iota(jnp.int32, (SPAN, count), 0).astype(f32)

    def group(g, _):
        four = []
        for bl in range(per):
            at = pl.ds(g, 1)
            i = fields[bl, a, at, :]
            j = fields[bl, rows + a, at, :]
            v = fields[bl, 2 * rows + a, at, :]
            left_hot = jnp.where(spot == i, v, 0.0).astype(bf)
            right_hot = jnp.where(spot == j, 1.0, 0.0).astype(bf)
            four.append(lax.dot_general(left_hot, right_hot, NT, preferred_element_type=f32))
        co4[pl.ds(pl.multiple_of(g * SPAN, SPAN), SPAN), :] = jnp.concatenate(four, axis=1).astype(bf)
        return 0

    lax.fori_loop(0, groups, group, 0, unroll=16)
    mid[...] = jnp.dot(co4[...], cb_ref[...], preferred_element_type=f32).astype(bf)
    step = per * SPAN
    for g in range(groups):
        cols = slice(g * step, (g + 1) * step)
        block = jnp.dot(ct_ref[...], mid[g * SPAN : (g + 1) * SPAN, :], preferred_element_type=f32)
        update = block.astype(bf)
        upv[:, cols] = update
        newv[:, cols] = (wv[:, cols].astype(f32) - LEARN_RATE * update.astype(f32)).astype(bf)


def decode(base, end, comp, w, before=()):
    replicas = sum(v.shape[0] for v in comp)
    width = w.shape[1]
    rows = w.shape[0] // SPAN
    per = 128 // TOPK
    groups = width // SPAN // per
    cos = cosine_table(SPAN)
    cb = jnp.asarray(cos, jnp.bfloat16)
    ct = jnp.asarray(cos.T / replicas, jnp.bfloat16)
    whole = lambda v: pl.BlockSpec(v.shape, lambda a: (0,) * v.ndim)
    wide = pl.BlockSpec((SPAN, width), lambda a: (a + base, 0))
    any_spec = pl.BlockSpec(memory_space=pl.ANY)
    out = jax.ShapeDtypeStruct(w.shape, jnp.bfloat16)
    bf = jnp.bfloat16
    return pl.pallas_call(
        functools.partial(decode_kernel, base),
        grid=(end - base,),
        in_specs=[*[whole(v) for v in comp], wide, whole(cb), whole(ct)] + [any_spec] * len(before),
        input_output_aliases={len(comp) + 3 + n: n for n in range(len(before))},
        out_specs=[wide, wide],
        out_shape=[out, out],
        scratch_shapes=[
            pltpu.VMEM((per * SPAN, per * SPAN), bf),
            pltpu.VMEM((per, 3 * rows, groups, replicas * TOPK), jnp.float32),
            pltpu.VMEM((groups * SPAN, per * SPAN), bf),
            pltpu.VMEM((groups * SPAN, per * SPAN), bf),
        ],
        cost_estimate=pl.CostEstimate(flops=8 << 30, bytes_accessed=12 << 20, transcendentals=0),
    )(*comp, w, cb, ct, *before)


def everyones_components(comp_index, comp_value):
    index = comp_index[0]
    mine = jnp.concatenate(
        [(index // SPAN).astype(jnp.bfloat16), (index % SPAN).astype(jnp.bfloat16), comp_value[0]], axis=0
    )
    mine = mine.reshape(-1, 128)
    pair = jnp.stack([mine, lax.ppermute(mine, "rep", TO_HI)])
    return [pair] + [lax.ppermute(pair, "rep", to) for to in (TO_UP, TO_DOWN, TO_FAR)]


def body(residual, gate_pre, up_pre, down_weight, d_out, comp_index, comp_value):
    t = lax.axis_index("tp")
    z, x, c = t // (2 * N_X), (t // 2) % N_X, t % 2
    y = lax.axis_index("rep") // 2
    gate_t = jnp.swapaxes(gate_pre[0], 0, 1)
    up_t = jnp.swapaxes(up_pre[0], 0, 1)
    w = down_weight
    quarter = w.shape[0] // N_Y
    own = d_out[0]

    steps = ((0, 0), (1, 0), (0, 3), (0, 1), (0, 2), (1, 3), (1, 1), (1, 2))
    spots = jnp.stack(
        [(z if dz == 0 else 1 - z) * N_X + (x + dx) % N_X for dz, dx in steps]
        + [c, z]
        + [((x + r) % N_X) * 2 + c for r in (2, 1, 3, 0)]
        + [(y + q) % N_Y for q in (0, 3, 1, 2)]
    ).astype(jnp.int32)

    from_z = over_z(own)
    from_l = right(own)
    from_r = left(own)
    own_p = swap(own)
    w_q0 = lax.ppermute(lax.dynamic_slice_in_dim(w, y * quarter, quarter, 0), ("rep", "tp"), TO_BACK)
    far_q = (y + N_Y // 2) % N_Y
    w_q2 = lax.ppermute(lax.dynamic_slice_in_dim(w, far_q * quarter, quarter, 0), ("rep", "tp"), TO_BACK)
    w_p = swap(w)
    comp = everyones_components(comp_index, comp_value)
    hid_other, hid_own = hidden_halves(spots, gate_t, up_t)
    hz = over_z(hid_other)
    hs_p = swap(hid_own)
    hz_p = swap(hz)

    span_rows = w.shape[0] // SPAN
    early = 2
    update, updated = decode(0, early, comp, w)
    update, updated = decode(early, span_rows, comp, w, (update, updated))

    half_rows = TOK // 2
    cut_a = from_l[:half_rows]
    cut_b = from_r[half_rows:]
    far_a = right(cut_a)
    far_b = left(cut_b)
    from_zl = right(from_z)
    from_zr = left(from_z)
    from_zfar_a = over_z(far_a)
    from_zfar_b = over_z(far_b)

    near = [[own], [own_p], [from_z], [swap(from_z)]]
    near += [[from_l], [swap(from_l)], [from_r], [swap(from_r)]]
    before = grads(0, spots, near, w, gate_t, up_t)
    rest = [[far_a, far_b], [swap(far_a), swap(far_b)]]
    rest += [[from_zl], [swap(from_zl)], [from_zr], [swap(from_zr)]]
    rest += [[from_zfar_a, from_zfar_b], [swap(from_zfar_a), swap(from_zfar_b)]]
    weight_grad, pre_grad, up_grad = grads(
        4, spots, rest, w, gate_t, up_t, before
    )

    width = w.shape[1] // 2
    w_qm = lax.ppermute(w_q0, "rep", TO_UP)
    w_qp = lax.ppermute(w_q0, "rep", TO_DOWN)
    w_back = [w_q0, w_qm, w_qp, w_q2]
    weights = [w, w_p, *w_back, *[swap(v) for v in w_back]]
    (a2, a1, a3, a0), (b2, b1, b3, b0) = forward(spots, (hid_own, hs_p, hz, hz_p), weights)
    f32 = jnp.float32

    ra = right(a2)
    rb = left(b2)
    ga = left(a3)
    gb = right(b1)
    sum_a = (a1.astype(f32) + ra.astype(f32)).astype(jnp.bfloat16)
    sum_b = (b3.astype(f32) + rb.astype(f32)).astype(jnp.bfloat16)
    fa = right(sum_a)
    fb = left(sum_b)
    res = residual[0]
    out_a = res[:, :width].astype(f32) + a0.astype(f32) + ga.astype(f32) + fa.astype(f32)
    out_b = res[:, width:].astype(f32) + b0.astype(f32) + gb.astype(f32) + fb.astype(f32)
    output = jnp.concatenate([out_a, out_b], axis=1).astype(jnp.bfloat16)
    return (
        output[None],
        jnp.swapaxes(pre_grad, 0, 1)[None],
        jnp.swapaxes(up_grad, 0, 1)[None],
        weight_grad[None],
        update,
        updated,
    )


def solution(mesh):
    return jax.shard_map(
        body,
        mesh=mesh,
        in_specs=(
            P("rep", "tp", None),
            P("rep", None, "tp"),
            P("rep", None, "tp"),
            P("tp", None),
            P("rep", "tp", None),
            P("rep", "tp", None),
            P("rep", "tp", None),
        ),
        out_specs=(
            P("rep", "tp", None),
            P("rep", None, "tp"),
            P("rep", None, "tp"),
            P("rep", "tp", None),
            P("tp", None),
            P("tp", None),
        ),
        check_vma=False,
    )
```
